32 devices in a mesh: gy: 8 (over z, y), gz: 4 (over x, core).
Axes of the slice: x: 2, y: 2, z: 4, core: 2. Of those that a mesh axis runs over, the one named last changes fastest.
Arguments:
- eddy_cells: int32 [8, 4, 2, 2048], P('gy', 'gz'), may hold values from 0 to 16383, as said below
- eddy_signs: int32 [8, 4, 3, 2048], P('gy', 'gz'), may hold values from -1 to 1, as said below
- eddy_counts: int32 [8, 4], P('gy', 'gz'), may hold values from 256 to 2048
- stress_diag: float32 [3, 16384], P(None, 'gy'), may hold values from 0.3 to 3
- stress_shear: float32 [3, 16384], P(None, 'gy'), may hold values from -3 to 3
- mean_flow: float32 [3, 16384, 1024], P(None, 'gy', 'gz'), may hold values from -6 to 6
Outputs:
- velocity: float32 [3, 16384, 1024], P(None, 'gy', 'gz')
The draws below stay inside these ranges and needn't reach their ends.
Inputs may be any that keep to these rules, and one draw needn't show every extreme that they name: `eddy_cells`: every slot of tile (i, j) holds a wall-normal cell in [i * 2048, (i + 1) * 2048) and a spanwise cell in [j * 256, (j + 1) * 256); only the first eddy_counts[i, j] slots are eddies. `eddy_signs`: each entry is -1 or 1.
All inputs are finite; a program needn't handle non-finite values.
Results may differ from the reference program's by a relative error of at most 0.0001.
Values sent between devices are 32-bit elements; how exact they have to be, the bound alone decides.
No kernel may reach another device: no remote copies, remote signals or barrier semaphores. Data moves between devices by JAX's collectives and lax.ppermute only.
A program may use at most 128 MiB of HBM per device.

```python
import math
import jax
import jax.numpy as jnp
from jax import lax

TY = 2048
TZ = 256
CAP = 2048
HALF = 128
TILES_Y = 8
TILES_Z = 4
NY = 16384
NZ = 1024


def draw_eddy_counts(key, part):
    rows_index = jnp.arange(TILES_Y, dtype=jnp.int32)
    highest = CAP - 3 * CAP // 4 * rows_index // max(TILES_Y - 1, 1)
    lowest = highest // 2
    key_counts, key_full = jax.random.split(jax.random.fold_in(key, 11))
    spread = jax.random.randint(key_counts, (TILES_Y, TILES_Z), 0, 1 << 20)
    counts = lowest[:, None] + spread % (highest - lowest + 1)[:, None]
    full_tile = jax.random.randint(key_full, (), 0, TILES_Z)
    counts = counts.at[0, full_tile].set(CAP)
    return counts.astype(jnp.int32)


def draw_eddy_cells(key, part):
    key_wall, key_span = jax.random.split(jax.random.fold_in(key, 23))
    wall_cells = jax.random.randint(key_wall, (TILES_Y, TILES_Z, CAP), 0, TY)
    wall_cells = wall_cells + (jnp.arange(TILES_Y, dtype=jnp.int32) * TY)[:, None, None]
    span_cells = jax.random.randint(key_span, (TILES_Y, TILES_Z, CAP), 0, TZ)
    span_cells = span_cells + (jnp.arange(TILES_Z, dtype=jnp.int32) * TZ)[None, :, None]
    return jnp.stack([wall_cells, span_cells], axis=2).astype(jnp.int32)


def draw_eddy_signs(key, part):
    coins = jax.random.randint(jax.random.fold_in(key, 37), (TILES_Y, TILES_Z, 3, CAP), 0, 2)
    return (coins * 2 - 1).astype(jnp.int32)


def level_of(stream_key, dims, pieces, least, largest):
    level = 1.0
    for dim, blocks in pieces:
        draws = jax.random.uniform(jax.random.fold_in(jax.random.fold_in(stream_key, 6), dim), (blocks,), jnp.float32, least / len(pieces), largest / len(pieces))
        level = level * jnp.repeat(jnp.exp(draws), dims[dim] // blocks).reshape((-1,) + (1,) * (len(dims) - 1 - dim))
    return level


def normal_values(own_key, extent, scale, most, cuts=(), held_as=jnp.bfloat16):
    gain = level_of(own_key, extent, cuts, -0.22, 0.18) if cuts else 1.0
    entries = jax.random.normal(own_key, extent, jnp.float32) * scale * gain
    return jnp.minimum(jnp.maximum(entries, -most), most).astype(held_as)


def setup_inputs(seed: int = 0) -> dict:
    key_list = jax.random.split(jax.random.key(seed), 7)
    return {
        "eddy_cells": draw_eddy_cells(jax.random.fold_in(key_list[6], 71), 0),
        "eddy_signs": draw_eddy_signs(jax.random.fold_in(key_list[6], 71), 0),
        "eddy_counts": draw_eddy_counts(jax.random.fold_in(key_list[6], 71), 0),
        "stress_diag": jnp.clip(jnp.exp(math.log(3.0) - 2.3025851 * jax.random.uniform(key_list[3], (3, NY), jnp.float32) ** level_of(key_list[3], (3, NY), ((1, 8),), -0.2, 0.2)), 0.3, 3.0),
        "stress_shear": normal_values(key_list[4], (3, NY), 0.5, 3.0, ((1, 8),), jnp.float32),
        "mean_flow": normal_values(key_list[5], (3, NY, NZ), 1.0, 6.0, ((1, 8), (2, 4)), jnp.float32),
    }


shape_peak = math.sqrt(1.5)

def profile(offsets):
    return shape_peak * jnp.maximum(1.0 - jnp.abs(offsets).astype(jnp.float32) / HALF, 0.0)

def tile_field(positions, signs_here, live_count, row_anchor, col_anchor, block_count):
    block_size = min(256, CAP)
    ext_rows = TY + 2 * HALF
    ext_cols = TZ + 2 * HALF
    row_cells = row_anchor - HALF + jnp.arange(ext_rows, dtype=jnp.int32)
    col_cells = col_anchor - HALF + jnp.arange(ext_cols, dtype=jnp.int32)

    def add_block(block_index, running):
        first_slot = (block_index * block_size).astype(jnp.int32)
        slot_index = first_slot + jnp.arange(block_size, dtype=jnp.int32)
        places = lax.dynamic_slice_in_dim(positions, first_slot, block_size, 1)
        weights = lax.dynamic_slice_in_dim(signs_here, first_slot, block_size, 1).astype(jnp.float32)
        weights = weights * (slot_index < live_count).astype(jnp.float32)[None, :]
        wall_profile = profile(row_cells[:, None] - places[0][None, :])
        span_profile = profile(col_cells[:, None] - places[1][None, :])
        signed = (weights[:, None, :] * wall_profile[None, :, :]).reshape(3 * ext_rows, block_size)
        return running + lax.dot_general(signed, span_profile, (((1,), (1,)), ((), ())), precision=lax.Precision.HIGHEST, preferred_element_type=jnp.float32)
    initial = jnp.zeros((3 * ext_rows, ext_cols), jnp.float32)
    return lax.fori_loop(jnp.int32(0), block_count, add_block, initial).reshape(3, ext_rows, ext_cols)

def rescale(raw_field, stress_diag, stress_shear, mean_flow, amplitude):
    streamwise = stress_diag[0][:, None] * raw_field[0]
    normal_part = stress_shear[0][:, None] * raw_field[0] + stress_diag[1][:, None] * raw_field[1]
    spanwise = stress_shear[1][:, None] * raw_field[0] + stress_shear[2][:, None] * raw_field[1] + stress_diag[2][:, None] * raw_field[2]
    return mean_flow + amplitude * jnp.stack([streamwise, normal_part, spanwise])

def reference(eddy_cells, eddy_signs, eddy_counts, stress_diag, stress_shear, mean_flow):
    block_count = CAP // min(256, CAP)
    canvas_init = jnp.zeros((3, NY + 2 * HALF, NZ + 2 * HALF), jnp.float32)

    def add_tile(tile_index, canvas):
        tile_row = (tile_index // TILES_Z).astype(jnp.int32)
        tile_col = (tile_index % TILES_Z).astype(jnp.int32)
        positions = lax.dynamic_index_in_dim(lax.dynamic_index_in_dim(eddy_cells, tile_row, 0, False), tile_col, 0, False)
        signs_here = lax.dynamic_index_in_dim(lax.dynamic_index_in_dim(eddy_signs, tile_row, 0, False), tile_col, 0, False)
        live_count = lax.dynamic_index_in_dim(lax.dynamic_index_in_dim(eddy_counts, tile_row, 0, False), tile_col, 0, False)
        extended = tile_field(positions, signs_here, live_count, tile_row * TY, tile_col * TZ, block_count)
        anchor = (jnp.int32(0), (tile_row * TY).astype(jnp.int32), (tile_col * TZ).astype(jnp.int32))
        current = lax.dynamic_slice(canvas, anchor, extended.shape)
        return lax.dynamic_update_slice(canvas, current + extended, anchor)
    canvas = lax.fori_loop(jnp.int32(0), jnp.int32(TILES_Y * TILES_Z), add_tile, canvas_init)
    inside = canvas[:, HALF:HALF + NY, :]
    middle = inside[:, :, HALF:HALF + NZ]
    middle = middle.at[:, :, :HALF].add(inside[:, :, NZ + HALF:])
    middle = middle.at[:, :, NZ - HALF:].add(inside[:, :, :HALF])
    eddy_total = jnp.sum(eddy_counts).astype(jnp.float32)
    amplitude = jnp.sqrt(NY * NZ / (HALF * HALF) / eddy_total)
    return rescale(middle, stress_diag, stress_shear, mean_flow, amplitude)
```

```python
import functools

import jax
import jax.numpy as jnp
from jax import lax
from jax.experimental import pallas as pl
from jax.experimental.pallas import tpu as pltpu
from jax.sharding import PartitionSpec as P


HALF = 128
ROWS = 512
CHUNK = 1024
KNOWN, COUNT = 5, 6


def pairs_near(size):
    return [(i, i ^ 1) for i in range(size)]


def pairs_far(size):
    return [(i, (i + 1 if i % 2 else i - 1) % size) for i in range(size)]


def pairs_inner(size):
    return [(i, i + 1 if i % 2 else i - 1) for i in range(1, size - 1)]


def pairs_over(size, by):
    return [(i, i ^ by) for i in range(size)]


def pairs_skip(size):
    skips, by = [], 4
    while by < size:
        skips.append(pairs_over(size, by))
        by *= 2
    return skips


def covers(rounds, size):
    known = [{i} for i in range(size)]
    for pairs in rounds:
        known = [known[i] | known[dict(pairs)[i]] for i in range(size)]
    return size > 2 and all(len(k) == size for k in known)


def whole(values):
    return values.astype(jnp.float32).astype(jnp.bfloat16)


def cells_of(nrows, ncols):
    cells = whole(lax.broadcasted_iota(jnp.int32, (nrows, HALF), 0) - HALF)
    return jnp.concatenate([cells] * (ncols // HALF), axis=1)


def tent(cells, places, origin):
    near = whole(jnp.clip(places - (origin + HALF), -2 * HALF, 2 * HALF))
    return jnp.maximum(HALF - jnp.abs(cells - near), 0).astype(jnp.bfloat16)


def wall_profiles(tile, row, nrows):
    step = min(nrows, 2 * HALF)
    cells = cells_of(step, tile.shape[1])
    return jnp.concatenate([tent(cells, tile[0:1, :], row + r) for r in range(0, nrows, step)], axis=0)


def chunks_of(slots):
    return (slots + CHUNK - 1) // CHUNK


def at_chunk(k):
    return pl.ds(pl.multiple_of(k * CHUNK, CHUNK), CHUNK)


def contract(a, b):
    return lax.dot_general(a, b, (((1,), (1,)), ((), ())), preferred_element_type=jnp.float32)


def fill_span(tile_ref, span_ref, slots, column):
    ncols = span_ref.shape[0] // 3

    def fill_chunk(k, carry):
        tile = tile_ref[:, at_chunk(k)]
        span = tent(cells_of(ncols, CHUNK), tile[1:2, :], column)
        signs = whole(tile[2:5, :])
        for c in range(3):
            span_ref[c * ncols : (c + 1) * ncols, at_chunk(k)] = span * signs[c : c + 1, :]
        return carry

    lax.fori_loop(0, chunks_of(slots), fill_chunk, 0)


def add_tile(out, tile_ref, span_ref, slots, row, column):
    ncols = span_ref.shape[0] // 3

    def add_chunk(k, carry):
        part = contract(wall_profiles(tile_ref[:, at_chunk(k)], row, ROWS), span_ref[:, at_chunk(k)])
        for c in range(3):
            out[c, :, pl.ds(column, ncols)] += part[:, c * ncols : (c + 1) * ncols]
        return carry

    lax.fori_loop(0, chunks_of(slots), add_chunk, 0)


def add_edge(out, tiles_ref, row, at_row, even_z):
    cols = out.shape[-1]

    def add(t, carry):
        tile = tiles_ref[t]
        column = jnp.where(even_z == 1, (1 - t) * cols, (t - 1) * cols)
        wall = wall_profiles(tile, row, HALF)
        signs = whole(tile[2:5, :])
        part = contract(
            jnp.concatenate([wall * signs[c : c + 1, :] for c in range(3)], axis=0),
            tent(cells_of(cols, tile.shape[1]), tile[1:2, :], column),
        )
        for c in range(3):
            out[c, pl.ds(at_row, HALF), :] += part[c * HALF : (c + 1) * HALF, :]
        return carry

    lax.fori_loop(0, 3, add, 0)


def edge_of(below, rows):
    return jnp.where(below == 1, -HALF, rows), pl.multiple_of(below * (ROWS - HALF), HALF)


def own_kernel(heads, tile, *refs, first):
    out, span = refs[-2:]
    block = pl.program_id(0)

    @pl.when(block == 0)
    def _():
        fill_span(tile, span, heads[COUNT, 0], 0)

    out[...] = jnp.zeros_like(out)
    add_tile(out, tile, span, heads[COUNT, 0], first + block * ROWS, 0)


def side_of(side, ncols):
    return jnp.where(side == 1, -ncols, 2 * ncols), pl.multiple_of(side * ncols, ncols)


def side_kernel(heads, own, tile, field, out, span):
    block = pl.program_id(0)
    ncols = span.shape[0] // 3
    origin, column = side_of(1 - own[COUNT, 2] % 2, ncols)

    @pl.when(block == 0)
    def _():
        fill_span(tile, span, heads[COUNT, 0], origin)

    out[...] = field[...]
    add_tile(out, tile, span, heads[COUNT, 0], block * ROWS, column)


def edge_kernel(own, tiles, out, *, rows):
    row, _ = edge_of(1 - own[COUNT, 1] % 2, rows)
    out[...] = jnp.zeros_like(out)
    add_edge(out, tiles, row, 0, 1 - own[COUNT, 2] % 2)


def last_kernel(heads, own, side, far, known, edge, diag, shear, mean, field, out, span, acc, *, rows, tiles_y, scale):
    block = pl.program_id(0)
    nblocks = rows // ROWS
    ncols = span.shape[0] // 3
    at_y, odd_z = own[COUNT, 1], own[COUNT, 2] % 2
    odd_y = at_y % 2
    origin, column = side_of(odd_z, ncols)
    acc[...] = field[...]

    @pl.when(block == 0)
    def _():
        fill_span(side, span, heads[COUNT, 0], origin)

    add_tile(acc, side, span, heads[COUNT, 0], block * ROWS, column)

    @pl.when(block == (1 - odd_y) * (nblocks - 1))
    def _():
        _, at_row = edge_of(1 - odd_y, rows)
        acc[:, pl.ds(at_row, HALF), :] += edge[...]

    @pl.when((block == odd_y * (nblocks - 1)) & (at_y > 0) & (at_y < tiles_y - 1))
    def _():
        row, at_row = edge_of(odd_y, rows)
        add_edge(acc, far, row, at_row, 1 - odd_z)

    total = jnp.sum(known[...].astype(jnp.float32), axis=1, keepdims=True)
    amplitude = jnp.sqrt(scale / total) * (1.5 / (HALF * HALF))
    factors = jnp.concatenate([diag[...], shear[...], jnp.zeros((2, ROWS), jnp.float32)], axis=0) * amplitude
    factors = factors.T
    a0, a1, a2 = (factors[:, k : k + 1] for k in range(3))
    b0, b1, b2 = (factors[:, 3 + k : 4 + k] for k in range(3))
    out[0] = mean[0] + a0 * acc[0]
    out[1] = mean[1] + (b0 * acc[0] + a1 * acc[1])
    out[2] = mean[2] + (b1 * acc[0] + b2 * acc[1] + a2 * acc[2])


def with_known(tile, known):
    return jnp.where(jnp.arange(tile.shape[0])[:, None] == KNOWN, known[None], tile)


def packed(places, signs, count, at_y, at_z, number):
    slots = places.shape[-1]
    slot = jnp.arange(slots, dtype=jnp.int32)[None]
    row = jnp.arange(8, dtype=jnp.int32)[:, None]
    signs = jnp.where(slot < count, signs, 0)
    known = jnp.where((row == KNOWN) & (slot == number), count, 0)
    place = jnp.where(slot == 0, count, jnp.where(slot == 1, at_y, at_z))
    rest = known + jnp.where(row == COUNT, place, 0)
    return jnp.pad(places, ((0, 6), (0, 0))) + jnp.pad(signs, ((2, 3), (0, 0))) + rest


def body(eddy_cells, eddy_signs, eddy_counts, stress_diag, stress_shear, mean_flow):
    slots = eddy_cells.shape[-1]
    _, rows, cols = mean_flow.shape
    tiles_y, tiles_z = lax.axis_size("gy"), lax.axis_size("gz")
    at_y, at_z = lax.axis_index("gy"), lax.axis_index("gz")
    assert cols == 2 * HALF and rows % (2 * ROWS) == 0 and tiles_y * tiles_z <= slots and slots % CHUNK == 0
    assert covers([pairs_near(tiles_z), pairs_far(tiles_z)] + pairs_skip(tiles_z), tiles_z)
    assert covers(pairs_skip(tiles_y) + [pairs_near(tiles_y), pairs_over(tiles_y, 2)], tiles_y)

    vmem = pl.BlockSpec(memory_space=pltpu.VMEM)
    anywhere = pl.BlockSpec(memory_space=pl.ANY)
    heads = pl.BlockSpec((8, HALF), lambda i: (0, 0), memory_space=pltpu.SMEM)
    field_block = pl.BlockSpec((3, ROWS, cols), lambda i: (0, i, 0))
    field_shape = jax.ShapeDtypeStruct((3, rows, cols), jnp.float32)
    own_span = pltpu.VMEM((3 * cols, slots), jnp.bfloat16)
    side_span = pltpu.VMEM((3 * HALF, slots), jnp.bfloat16)
    macs = 3 * rows * cols * slots

    def cost(part, moved):
        return pl.CostEstimate(flops=int(2 * macs * part), transcendentals=0, bytes_accessed=int(4 * moved * 3 * rows * cols))

    def own_part(first, tile, field=None):
        return pl.pallas_call(
            functools.partial(own_kernel, first=first),
            grid=(rows // ROWS // 2,),
            in_specs=[heads, vmem] + ([] if field is None else [anywhere]),
            out_specs=pl.BlockSpec((3, ROWS, cols), lambda i: (0, i + first // ROWS, 0)),
            out_shape=field_shape,
            scratch_shapes=[own_span],
            input_output_aliases={} if field is None else {2: 0},
            cost_estimate=cost(0.5, 0.5),
        )(tile, tile, *([] if field is None else [field]))

    anchor = jnp.stack([at_y * rows, at_z * cols]).astype(jnp.int32)
    places = eddy_cells.reshape(2, slots) - anchor[:, None]
    own = packed(places, eddy_signs.reshape(3, slots), eddy_counts.reshape(()), at_y, at_z, at_y * tiles_z + at_z)

    near_z = lax.ppermute(own, "gz", pairs_near(tiles_z))
    known = jnp.maximum(own[KNOWN], near_z[KNOWN])
    far_z = lax.ppermute(with_known(own, known), "gz", pairs_far(tiles_z))
    field = own_part(0, own)
    known = jnp.maximum(known, far_z[KNOWN])
    for pairs in pairs_skip(tiles_z):
        known = jnp.maximum(known, lax.ppermute(known, "gz", pairs))
    for pairs in pairs_skip(tiles_y):
        known = jnp.maximum(known, lax.ppermute(known, "gy", pairs))
    field = own_part(rows // 2, own, field)
    row_of_tiles = jnp.stack([far_z, with_known(own, known), near_z])
    near_y = lax.ppermute(row_of_tiles, "gy", pairs_near(tiles_y))
    far_y = lax.ppermute(row_of_tiles, "gy", pairs_inner(tiles_y))
    field = pl.pallas_call(
        side_kernel,
        grid=(rows // ROWS,),
        in_specs=[heads, heads, vmem, field_block],
        out_specs=field_block,
        out_shape=field_shape,
        scratch_shapes=[side_span],
        input_output_aliases={3: 0},
        cost_estimate=cost(0.7, 2.0),
    )(near_z, own, near_z, field)
    known = jnp.maximum(known, near_y[1, KNOWN])
    over = lax.ppermute(known, "gy", pairs_over(tiles_y, 2))
    known = jnp.maximum(known, over)[None]
    edge = pl.pallas_call(
        functools.partial(edge_kernel, rows=rows),
        grid=(1,),
        in_specs=[heads, vmem],
        out_specs=vmem,
        out_shape=jax.ShapeDtypeStruct((3, HALF, cols), jnp.float32),
        cost_estimate=cost(0.2, 0.1),
    )(own, near_y)

    stress_block = pl.BlockSpec((3, ROWS), lambda i: (0, i))
    scale = rows * tiles_y * (cols * tiles_z) / (HALF * HALF)
    return pl.pallas_call(
        functools.partial(last_kernel, rows=rows, tiles_y=tiles_y, scale=scale),
        grid=(rows // ROWS,),
        in_specs=[heads, heads, vmem, vmem, vmem, vmem, stress_block, stress_block, field_block, field_block],
        out_specs=field_block,
        out_shape=field_shape,
        scratch_shapes=[side_span, pltpu.VMEM((3, ROWS, cols), jnp.float32)],
        cost_estimate=cost(0.5, 3.0),
    )(far_z, own, far_z, far_y, known, edge, stress_diag, stress_shear, mean_flow, field)


def solution(mesh):
    in_specs = (
        P("gy", "gz", None, None),
        P("gy", "gz", None, None),
        P("gy", "gz"),
        P(None, "gy"),
        P(None, "gy"),
        P(None, "gy", "gz"),
    )

    return jax.shard_map(body, mesh=mesh, in_specs=in_specs, out_specs=P(None, "gy", "gz"), check_vma=False)
```

```python
import functools

import jax
import jax.numpy as jnp
from jax import lax
from jax.experimental import pallas as pl
from jax.experimental.pallas import tpu as pltpu
from jax.sharding import PartitionSpec as P


HALF = 128
ROWS = 512
LAST_ROWS = 256
WINDOW = 512
EDGE_WINDOW = 256
SORT = 256
KNOWN, HEAD, START = 5, 6, 3


def pairs_near(size):
    return [(i, i ^ 1) for i in range(size)]


def pairs_far(size):
    return [(i, (i + 1 if i % 2 else i - 1) % size) for i in range(size)]


def pairs_inner(size):
    return [(i, i + 1 if i % 2 else i - 1) for i in range(1, size - 1)]


def pairs_over(size, by):
    return [(i, i ^ by) for i in range(size)]


def pairs_skip(size):
    skips, by = [], 4
    while by < size:
        skips.append(pairs_over(size, by))
        by *= 2
    return skips


def covers(rounds, size):
    known = [{i} for i in range(size)]
    for pairs in rounds:
        known = [known[i] | known[dict(pairs)[i]] for i in range(size)]
    return size > 2 and all(len(k) == size for k in known)


def whole(values):
    return values.astype(jnp.float32).astype(jnp.bfloat16)


def cells_of(nrows, ncols):
    cells = whole(lax.broadcasted_iota(jnp.int32, (nrows, HALF), 0) - HALF)
    return jnp.concatenate([cells] * (ncols // HALF), axis=1)


def tent(cells, places, origin):
    near = whole(jnp.clip(places - (origin + HALF), -2 * HALF, 2 * HALF))
    return jnp.maximum(HALF - jnp.abs(cells - near), 0).astype(jnp.bfloat16)


def wall_profiles(tile, row, nrows):
    step = min(nrows, 2 * HALF)
    cells = cells_of(step, tile.shape[1])
    return jnp.concatenate([tent(cells, tile[0:1, :], row + r) for r in range(0, nrows, step)], axis=0)


def contract(a, b):
    return lax.dot_general(a, b, (((1,), (1,)), ((), ())), preferred_element_type=jnp.float32)


def order_kernel(heads, tile, out, *, bands):
    slots = tile.shape[1]
    nbuckets = -(-(2 * bands + 1) // 16) * 16
    places = tile[0:2, :]
    slot = lax.broadcasted_iota(jnp.int32, (1, slots), 1)
    bucket = jnp.where(slot < heads[HEAD, 0], (places[1:2] >> 7) * bands + (places[0:1] >> 7), 2 * bands)
    ids = lax.broadcasted_iota(jnp.int32, (nbuckets, HALF), 0)
    wide_ids = jnp.concatenate([ids] * (slots // HALF), axis=1)
    starts = jnp.sum((bucket < wide_ids).astype(jnp.float32), axis=1, keepdims=True)
    member = jnp.maximum(1 - jnp.abs(whole(wide_ids) - whole(bucket)), 0).astype(jnp.bfloat16)
    upto = lax.broadcasted_iota(jnp.int32, (SORT, SORT), 0) <= lax.broadcasted_iota(jnp.int32, (SORT, SORT), 1)
    pieces = [member[:, k : k + SORT] for k in range(0, slots, SORT)]
    so_far = lax.dot_general(
        jnp.concatenate(pieces, axis=0),
        whole(upto.astype(jnp.int32)),
        (((1,), (0,)), ((), ())),
        preferred_element_type=jnp.float32,
    )
    base = starts - 1
    ranks = []
    for k, piece in enumerate(pieces):
        part = so_far[k * nbuckets : (k + 1) * nbuckets, :]
        ranks.append(jnp.sum(piece.astype(jnp.float32) * (part + base), axis=0, keepdims=True))
        base = base + part[:, SORT - 1 : SORT]
    rank = jnp.concatenate(ranks, axis=1).astype(jnp.int32)

    values = whole(jnp.concatenate([places[0:1] >> 7, places[0:1] & (HALF - 1), tile[1:5, :], tile[0:2, :] * 0], axis=0))
    cells = jnp.concatenate([whole(lax.broadcasted_iota(jnp.int32, (SORT, HALF), 0))] * (slots // HALF), axis=1)
    for k in range(slots // SORT):
        local = whole(jnp.where(rank // SORT == k, rank % SORT, -1))
        chosen = jnp.maximum(1 - jnp.abs(cells - local), 0).astype(jnp.bfloat16)
        got = contract(values, chosen).astype(jnp.int32)
        at = slice(k * SORT, (k + 1) * SORT)
        out[0:1, at] = got[0:1] * HALF + got[1:2]
        out[1:5, at] = got[2:6]
    out[KNOWN : KNOWN + 1, :] = tile[KNOWN : KNOWN + 1, :]
    out[HEAD:, :] = jnp.zeros((8 - HEAD, slots), jnp.int32)
    lane = lax.broadcasted_iota(jnp.int32, (nbuckets, HALF), 1)
    firsts = jnp.sum(jnp.where(lane == ids + START, starts, 0.0), axis=0, keepdims=True).astype(jnp.int32)
    out[HEAD : HEAD + 1, :HALF] = jnp.where(lane[0:1] < START, tile[HEAD : HEAD + 1, :HALF], firsts)


def slots_of(head, half, low, high, bands):
    return head(START + half * bands + low), head(START + half * bands + high + 1)


def profiles(tile_ref, first, span, origin, nrows, ncols, size, signed_wall):
    at = pl.multiple_of(jnp.minimum(first, tile_ref.shape[-1] - size), HALF)
    tile = tile_ref[:, pl.ds(at, size)]
    slot = at + lax.broadcasted_iota(jnp.int32, (1, size), 1)
    inside = (slot >= jnp.maximum(span[0], first)) & (slot < jnp.minimum(span[1], first + size))
    signs = whole(jnp.where(inside, tile[2:5, :], 0))
    wall = wall_profiles(tile, origin[0], nrows)
    along = tent(cells_of(ncols, size), tile[1:2, :], origin[1])
    if signed_wall:
        return jnp.concatenate([wall * signs[c : c + 1, :] for c in range(3)], axis=0), along
    return wall, jnp.concatenate([along * signs[c : c + 1, :] for c in range(3)], axis=0)


def add_windows(out, sources, firsts, at_row, nrows, at_col, ncols, size, signed_wall, base, base_row):
    pairs = [profiles(s[0], f, s[1], s[2], nrows, ncols, size, signed_wall) for s, f in zip(sources, firsts)]
    wall, along = (jnp.concatenate(x, axis=1) if len(x) > 1 else x[0] for x in zip(*pairs))
    part = contract(wall, along)
    for c in range(3):
        piece = part[c * nrows : (c + 1) * nrows] if signed_wall else part[:, c * ncols : (c + 1) * ncols]
        if base is not None:
            piece = piece + base[c, pl.ds(base_row, nrows), pl.ds(at_col, ncols)]
        out[c, pl.ds(at_row, nrows), pl.ds(at_col, ncols)] = piece


def first_window(source):
    return source[1][0] // HALF * HALF


def add_first(out, sources, at_row, nrows, at_col, ncols, size, signed_wall=False, base=None, base_row=0):
    firsts = [first_window(s) for s in sources]
    add_windows(out, sources, firsts, at_row, nrows, at_col, ncols, size, signed_wall, base, base_row)


def add_rest(out, sources, at_row, nrows, at_col, ncols, size, signed_wall=False):
    for source in sources:
        first = first_window(source)

        def more(k, carry, source=source, first=first):
            start = [first + k * size]
            add_windows(out, [source], start, at_row, nrows, at_col, ncols, size, signed_wall, out, at_row)
            return carry

        lax.fori_loop(1, (source[1][1] - first + size - 1) // size, more, 0)


def reach(row, bands):
    band = row // HALF
    return jnp.maximum(band - 1, 0), jnp.minimum(band + ROWS // HALF, bands - 1)


def head_of(heads):
    return lambda lane: heads[HEAD, lane]


def own_sources(heads, tile, row, bands):
    low, high = reach(row, bands)
    return [(tile, slots_of(head_of(heads), half, low, high, bands), (row, 0)) for half in range(2)]


def side_sources(heads, tile, side, row, ncols, bands):
    low, high = reach(row, bands)
    origin = jnp.where(side == 1, -ncols, 2 * ncols)
    return [(tile, slots_of(head_of(heads), 1 - side, low, high, bands), (row, origin))]


def add_edge(out, heads, tiles, below, even_z, bands):
    cols = out.shape[2]
    row = jnp.where(below == 1, -HALF, bands * HALF)
    band = jnp.where(below == 1, 0, bands - 1)
    sources = []
    for t, half in ((0, even_z), (1, 0), (1, 1), (2, 1 - even_z)):
        column = (1 - t) * (2 * even_z - 1) * cols
        span = slots_of(lambda lane, t=t: heads[t, HEAD, lane], half, band, band, bands)
        sources.append((tiles.at[t], span, (row, column)))
    at = (0, HALF, 0, cols, EDGE_WINDOW)
    add_first(out, sources, *at, signed_wall=True, base=out)
    add_rest(out, sources, *at, signed_wall=True)


def transform(diag, shear, part):
    factors = jnp.concatenate([diag, shear, jnp.zeros((2, diag.shape[1]), jnp.float32)], axis=0).T
    a0, a1, a2 = (factors[:, k : k + 1] for k in range(3))
    b0, b1, b2 = (factors[:, 3 + k : 4 + k] for k in range(3))
    return a0 * part[0], b0 * part[0] + a1 * part[1], b1 * part[0] + b2 * part[1] + a2 * part[2]


def own_kernel(own_heads, own, out, *, bands, first):
    cols = out.shape[2]

    def add_block(block, carry):
        row = pl.multiple_of(block * ROWS, ROWS)
        sources = own_sources(own_heads, own, first + row, bands)
        add_first(out, sources, row, ROWS, 0, cols, WINDOW)
        add_rest(out, sources, row, ROWS, 0, cols, WINDOW)
        return carry

    lax.fori_loop(0, out.shape[1] // ROWS, add_block, 0)


def field_kernel(own_heads, near_heads, far_heads, own, near, far, diag, shear, *refs, bands, first):
    *raw, out, acc = refs
    cols = out.shape[2]
    ncols = cols // 2
    odd_z = own_heads[HEAD, 2] % 2
    whole_at = (0, ROWS, 0, cols, WINDOW)
    near_at = (0, ROWS, pl.multiple_of((1 - odd_z) * ncols, ncols), ncols, WINDOW)
    far_at = (0, ROWS, pl.multiple_of(odd_z * ncols, ncols), ncols, WINDOW)

    def finish(block):
        at = pl.ds(pl.multiple_of(block * ROWS, ROWS), ROWS)
        at_factors = pl.ds(pl.multiple_of(first + block * ROWS, ROWS), ROWS)
        for c, part in enumerate(transform(diag[:, at_factors], shear[:, at_factors], acc)):
            out[c, at, :] = part

    def add_block(block, carry):
        row = pl.multiple_of(first + block * ROWS, ROWS)
        from_own = own_sources(own_heads, own, row, bands)
        from_near = side_sources(near_heads, near, 1 - odd_z, row, ncols, bands)
        from_far = side_sources(far_heads, far, odd_z, row, ncols, bands)
        finish(jnp.maximum(block - 1, 0))
        base, base_row = (raw[0], pl.multiple_of(block * ROWS, ROWS)) if raw else (acc, 0)
        if not raw:
            add_first(acc, from_own, *whole_at)
        add_first(acc, from_near, *near_at, base=base, base_row=base_row)
        add_first(acc, from_far, *far_at, base=base, base_row=base_row)
        if not raw:
            add_rest(acc, from_own, *whole_at)
        add_rest(acc, from_near, *near_at)
        add_rest(acc, from_far, *far_at)
        return carry

    nblocks = out.shape[1] // ROWS
    acc[...] = jnp.zeros_like(acc)
    lax.fori_loop(0, nblocks, add_block, 0)
    finish(nblocks - 1)


def last_kernel(
    own_heads, up_heads, down_heads, near_y, far_y, over, known, upper, lower, diag, shear, mean, out, acc,
    *, bands, tiles_y, scale
):
    block = pl.program_id(0)
    rows = out.shape[1]
    nblocks = bands * HALF // rows
    at_y, odd_z = own_heads[HEAD, 1], own_heads[HEAD, 2] % 2
    odd_y = at_y % 2
    total = jnp.sum(jnp.maximum(known[...], over[...]).astype(jnp.float32), axis=1, keepdims=True)
    amplitude = jnp.sqrt(scale / total) * (1.5 / (HALF * HALF))
    for part, held in enumerate((upper, lower)):

        @pl.when(block // (nblocks // 2) == part)
        def _(held=held):
            row = pl.multiple_of((block % (nblocks // 2)) * rows, rows)
            out[...] = mean[...] + amplitude * held[:, pl.ds(row, rows), :]

    def add_beyond(heads, tiles, below):
        acc[...] = jnp.zeros_like(acc)
        add_edge(acc, heads, tiles, below, 1 - odd_z, bands)
        first = pl.multiple_of(below * (bands * HALF - HALF), HALF)
        parts = transform(diag[:, pl.ds(first, HALF)], shear[:, pl.ds(first, HALF)], acc)
        at = pl.ds(pl.multiple_of(below * (rows - HALF), HALF), HALF)
        for c, part in enumerate(parts):
            out[c, at, :] += amplitude * part

    @pl.when(block == (1 - odd_y) * (nblocks - 1))
    def _():
        add_beyond(up_heads, near_y, 1 - odd_y)

    @pl.when((block == odd_y * (nblocks - 1)) & (at_y > 0) & (at_y < tiles_y - 1))
    def _():
        add_beyond(down_heads, far_y, odd_y)


def with_known(tile, known):
    wide = jnp.pad(known, ((0, 0), (0, tile.shape[1] - known.shape[1])))
    return jnp.where(jnp.arange(tile.shape[0])[:, None] == KNOWN, wide, tile)


def packed(places, signs, count, at_y, at_z):
    slots = places.shape[-1]
    slot = jnp.arange(slots, dtype=jnp.int32)[None]
    row = jnp.arange(8, dtype=jnp.int32)[:, None]
    signs = jnp.where(slot < count, signs, 0)
    place = jnp.where(slot == 0, count, jnp.where(slot == 1, at_y, at_z))
    rest = jnp.where(row == HEAD, place, 0)
    return jnp.pad(places, ((0, 6), (0, 0))) + jnp.pad(signs, ((2, 3), (0, 0))) + rest


def body(eddy_cells, eddy_signs, eddy_counts, stress_diag, stress_shear, mean_flow):
    slots = eddy_cells.shape[-1]
    _, rows, cols = mean_flow.shape
    tiles_y, tiles_z = lax.axis_size("gy"), lax.axis_size("gz")
    at_y, at_z = lax.axis_index("gy"), lax.axis_index("gz")
    assert cols == 2 * HALF and rows % (2 * ROWS) == 0 and slots % WINDOW == 0
    bands = rows // HALF
    assert START + 2 * bands < HALF
    assert tiles_z > 2 and tiles_z & (tiles_z - 1) == 0
    assert covers(pairs_skip(tiles_y) + [pairs_near(tiles_y), pairs_over(tiles_y, 2)], tiles_y)
    bands = rows // HALF
    assert START + 2 * bands < HALF
    assert covers([pairs_near(tiles_z), pairs_far(tiles_z)] + pairs_skip(tiles_z), tiles_z)
    assert covers(pairs_skip(tiles_y) + [pairs_near(tiles_y), pairs_over(tiles_y, 2)], tiles_y)

    vmem = pl.BlockSpec(memory_space=pltpu.VMEM)
    heads = pl.BlockSpec((8, HALF), lambda i: (0, 0), memory_space=pltpu.SMEM)
    field_block = pl.BlockSpec((3, ROWS, cols), lambda i: (0, i, 0))
    field_shape = jax.ShapeDtypeStruct((3, rows, cols), jnp.float32)
    edge_heads = pl.BlockSpec((3, 8, HALF), lambda i: (0, 0, 0), memory_space=pltpu.SMEM)
    macs = 3 * rows * cols * slots

    def cost(part, moved):
        return pl.CostEstimate(flops=int(2 * macs * part), transcendentals=0, bytes_accessed=int(4 * moved * 3 * rows * cols))

    count = eddy_counts.reshape(())
    lanes = -(-tiles_y * tiles_z // HALF) * HALF
    known = jnp.where(jnp.arange(lanes, dtype=jnp.int32)[None] == at_y * tiles_z + at_z, count, 0)
    anchor = jnp.stack([at_y * rows, at_z * cols]).astype(jnp.int32)
    places = eddy_cells.reshape(2, slots) - anchor[:, None]
    own = packed(places, eddy_signs.reshape(3, slots), count, at_y, at_z)
    known, own = lax.optimization_barrier((known, own))
    for pairs in pairs_skip(tiles_y):
        known = jnp.maximum(known, lax.ppermute(known, "gy", pairs))
    own = pl.pallas_call(
        functools.partial(order_kernel, bands=bands),
        grid=(1,),
        in_specs=[heads, vmem],
        out_specs=vmem,
        out_shape=jax.ShapeDtypeStruct((8, slots), jnp.int32),
        cost_estimate=cost(0.3, 0.1),
        compiler_params=pltpu.CompilerParams(vmem_limit_bytes=24 << 20),
    )(own, own)

    own = with_known(own, known)
    near_z = lax.ppermute(own, "gz", pairs_near(tiles_z))
    far_z = lax.ppermute(own, "gz", pairs_far(tiles_z))
    others = [known, near_z[KNOWN : KNOWN + 1, :lanes], far_z[KNOWN : KNOWN + 1, :lanes]]
    for by in range(2, tiles_z):
        if tiles_z != 4 or by == 2:
            others.append(lax.ppermute(known, "gz", pairs_over(tiles_z, by)))
    known = functools.reduce(jnp.maximum, others)
    row_of_tiles = jnp.stack([far_z, own, near_z])
    one = lax.ppermute(known, "gy", pairs_near(tiles_y))
    near_y = lax.ppermute(row_of_tiles, "gy", pairs_near(tiles_y))
    far_y = lax.ppermute(row_of_tiles, "gy", pairs_inner(tiles_y))

    half = rows // 2
    half_shape = jax.ShapeDtypeStruct((3, half, cols), jnp.float32)
    params = pltpu.CompilerParams(vmem_limit_bytes=24 << 20)
    acc = pltpu.VMEM((3, ROWS, cols), jnp.float32)
    raw = pl.pallas_call(
        functools.partial(own_kernel, bands=bands, first=0),
        grid=(1,),
        in_specs=[heads, vmem],
        out_specs=vmem,
        out_shape=half_shape,
        cost_estimate=cost(0.2, 0.5),
        compiler_params=params,
    )(own, own)

    def field_part(first, *raw):
        return pl.pallas_call(
            functools.partial(field_kernel, bands=bands, first=first),
            grid=(1,),
            in_specs=[heads] * 3 + [vmem] * (5 + len(raw)),
            out_specs=vmem,
            out_shape=half_shape,
            scratch_shapes=[acc],
            cost_estimate=cost(0.2, 0.5),
            compiler_params=params,
        )(own, near_z, far_z, own, near_z, far_z, stress_diag, stress_shear, *raw)

    lower = field_part(half)
    known = jnp.maximum(known, one)
    over = lax.ppermute(known, "gy", pairs_over(tiles_y, 2))
    upper = field_part(0, raw)

    block_rows = LAST_ROWS
    last_block = pl.BlockSpec((3, block_rows, cols), lambda i: (0, i, 0))
    scale = rows * tiles_y * (cols * tiles_z) / (HALF * HALF)
    return pl.pallas_call(
        functools.partial(last_kernel, bands=bands, tiles_y=tiles_y, scale=scale),
        grid=(rows // block_rows,),
        in_specs=[heads] + [edge_heads] * 2 + [vmem] * 8 + [last_block],
        out_specs=last_block,
        out_shape=field_shape,
        scratch_shapes=[pltpu.VMEM((3, HALF, cols), jnp.float32)],
        cost_estimate=cost(0.3, 2.0),
        compiler_params=pltpu.CompilerParams(vmem_limit_bytes=24 << 20),
    )(
        own, near_y, far_y, near_y, far_y, over, known, upper, lower,
        stress_diag, stress_shear, mean_flow,
    )


def solution(mesh):
    in_specs = (
        P("gy", "gz", None, None),
        P("gy", "gz", None, None),
        P("gy", "gz"),
        P(None, "gy"),
        P(None, "gy"),
        P(None, "gy", "gz"),
    )

    return jax.shard_map(body, mesh=mesh, in_specs=in_specs, out_specs=P(None, "gy", "gz"), check_vma=False)
```

```python
import functools

import jax
import jax.numpy as jnp
from jax import lax
from jax.experimental import pallas as pl
from jax.experimental.pallas import tpu as pltpu
from jax.sharding import PartitionSpec as P


HALF = 128
ROWS = 512
LAST_ROWS = 1024
WINDOW = 512
EDGE_WINDOW = 256
SORT = 256
KNOWN, HEAD, START = 5, 6, 3


def pairs_near(size):
    return [(i, i ^ 1) for i in range(size)]


def pairs_far(size):
    return [(i, (i + 1 if i % 2 else i - 1) % size) for i in range(size)]


def pairs_inner(size):
    return [(i, i + 1 if i % 2 else i - 1) for i in range(1, size - 1)]


def pairs_over(size, by):
    return [(i, i ^ by) for i in range(size)]


def pairs_skip(size):
    skips, by = [], 4
    while by < size:
        skips.append(pairs_over(size, by))
        by *= 2
    return skips


def covers(rounds, size):
    known = [{i} for i in range(size)]
    for pairs in rounds:
        known = [known[i] | known[dict(pairs)[i]] for i in range(size)]
    return size > 2 and all(len(k) == size for k in known)


def whole(values):
    return values.astype(jnp.float32).astype(jnp.bfloat16)


def cells_of(nrows, ncols):
    cells = whole(lax.broadcasted_iota(jnp.int32, (nrows, HALF), 0) - HALF)
    return jnp.concatenate([cells] * (ncols // HALF), axis=1)


def tent(cells, places, origin):
    near = whole(jnp.clip(places - (origin + HALF), -2 * HALF, 2 * HALF))
    return jnp.maximum(HALF - jnp.abs(cells - near), 0).astype(jnp.bfloat16)


def wall_profiles(tile, row, nrows):
    step = min(nrows, 2 * HALF)
    cells = cells_of(step, tile.shape[1])
    return jnp.concatenate([tent(cells, tile[0:1, :], row + r) for r in range(0, nrows, step)], axis=0)


def contract(a, b):
    return lax.dot_general(a, b, (((1,), (1,)), ((), ())), preferred_element_type=jnp.float32)


def order_kernel(count, cells, signs, out, *, bands, cols):
    slots = cells.shape[1]
    at_y, at_z = lax.axis_index("gy"), lax.axis_index("gz")
    nbuckets = -(-(2 * bands + 1) // 16) * 16
    places = jnp.concatenate([cells[0:1, :] - at_y * (bands * HALF), cells[1:2, :] - at_z * cols], axis=0)
    slot = lax.broadcasted_iota(jnp.int32, (1, slots), 1)
    bucket = jnp.where(slot < count[0, 0], (places[1:2] >> 7) * bands + (places[0:1] >> 7), 2 * bands)
    ids = lax.broadcasted_iota(jnp.int32, (nbuckets, HALF), 0)
    wide_ids = jnp.concatenate([ids] * (slots // HALF), axis=1)
    starts = jnp.sum((bucket < wide_ids).astype(jnp.float32), axis=1, keepdims=True)
    member = jnp.maximum(1 - jnp.abs(whole(wide_ids) - whole(bucket)), 0).astype(jnp.bfloat16)
    upto = lax.broadcasted_iota(jnp.int32, (SORT, SORT), 0) <= lax.broadcasted_iota(jnp.int32, (SORT, SORT), 1)
    pieces = [member[:, k : k + SORT] for k in range(0, slots, SORT)]
    so_far = lax.dot_general(
        jnp.concatenate(pieces, axis=0),
        whole(upto.astype(jnp.int32)),
        (((1,), (0,)), ((), ())),
        preferred_element_type=jnp.float32,
    )
    base = starts - 1
    ranks = []
    for k, piece in enumerate(pieces):
        part = so_far[k * nbuckets : (k + 1) * nbuckets, :]
        ranks.append(jnp.sum(piece.astype(jnp.float32) * (part + base), axis=0, keepdims=True))
        base = base + part[:, SORT - 1 : SORT]
    rank = jnp.concatenate(ranks, axis=1).astype(jnp.int32)

    live = jnp.where(slot < count[0, 0], signs[...], 0)
    parts = [places[0:1] >> 7, places[0:1] & (HALF - 1), places[1:2], live, jnp.zeros((2, slots), jnp.int32)]
    values = whole(jnp.concatenate(parts, axis=0))
    cells = jnp.concatenate([whole(lax.broadcasted_iota(jnp.int32, (SORT, HALF), 0))] * (slots // HALF), axis=1)
    for k in range(slots // SORT):
        local = whole(jnp.where(rank // SORT == k, rank % SORT, -1))
        chosen = jnp.maximum(1 - jnp.abs(cells - local), 0).astype(jnp.bfloat16)
        got = contract(values, chosen).astype(jnp.int32)
        at = slice(k * SORT, (k + 1) * SORT)
        out[0:1, at] = got[0:1] * HALF + got[1:2]
        out[1:5, at] = got[2:6]
    out[KNOWN:, :] = jnp.zeros((8 - KNOWN, slots), jnp.int32)
    lane = lax.broadcasted_iota(jnp.int32, (nbuckets, HALF), 1)
    firsts = jnp.sum(jnp.where(lane == ids + START, starts, 0.0), axis=0, keepdims=True).astype(jnp.int32)
    place = jnp.where(lane[0:1] == 0, count[0, 0], jnp.where(lane[0:1] == 1, at_y, at_z))
    out[HEAD : HEAD + 1, :HALF] = jnp.where(lane[0:1] < START, place, firsts)


def slots_of(head, half, low, high, bands):
    return head(START + half * bands + low), head(START + half * bands + high + 1)


def profiles(tile_ref, first, span, origin, nrows, ncols, size, signed_wall):
    at = pl.multiple_of(jnp.minimum(first, tile_ref.shape[-1] - size), HALF)
    tile = tile_ref[:, pl.ds(at, size)]
    slot = at + lax.broadcasted_iota(jnp.int32, (1, size), 1)
    inside = (slot >= jnp.maximum(span[0], first)) & (slot < jnp.minimum(span[1], first + size))
    signs = whole(jnp.where(inside, tile[2:5, :], 0))
    wall = wall_profiles(tile, origin[0], nrows)
    along = tent(cells_of(ncols, size), tile[1:2, :], origin[1])
    if signed_wall:
        return jnp.concatenate([wall * signs[c : c + 1, :] for c in range(3)], axis=0), along
    return wall, jnp.concatenate([along * signs[c : c + 1, :] for c in range(3)], axis=0)


def add_windows(out, sources, firsts, at_row, nrows, at_col, ncols, size, signed_wall, base, base_row):
    pairs = [profiles(s[0], f, s[1], s[2], nrows, ncols, size, signed_wall) for s, f in zip(sources, firsts)]
    wall, along = (jnp.concatenate(x, axis=1) if len(x) > 1 else x[0] for x in zip(*pairs))
    part = contract(wall, along)
    for c in range(3):
        piece = part[c * nrows : (c + 1) * nrows] if signed_wall else part[:, c * ncols : (c + 1) * ncols]
        if base is not None:
            piece = piece + base[c, pl.ds(base_row, nrows), pl.ds(at_col, ncols)]
        out[c, pl.ds(at_row, nrows), pl.ds(at_col, ncols)] = piece


def first_window(source):
    return source[1][0] // HALF * HALF


def add_first(out, sources, at_row, nrows, at_col, ncols, size, signed_wall=False, base=None, base_row=0):
    firsts = [first_window(s) for s in sources]
    add_windows(out, sources, firsts, at_row, nrows, at_col, ncols, size, signed_wall, base, base_row)


def add_rest(out, sources, at_row, nrows, at_col, ncols, size, signed_wall=False):
    for source in sources:
        first = first_window(source)

        def more(k, carry, source=source, first=first):
            start = [first + k * size]
            add_windows(out, [source], start, at_row, nrows, at_col, ncols, size, signed_wall, out, at_row)
            return carry

        lax.fori_loop(1, (source[1][1] - first + size - 1) // size, more, 0)


def reach(row, bands):
    band = row // HALF
    return jnp.maximum(band - 1, 0), jnp.minimum(band + ROWS // HALF, bands - 1)


def head_of(heads):
    return lambda lane: heads[HEAD, lane]


def own_sources(heads, tile, row, bands):
    low, high = reach(row, bands)
    return [(tile, slots_of(head_of(heads), half, low, high, bands), (row, 0)) for half in range(2)]


def side_sources(heads, tiles, place, side, row, ncols, bands):
    low, high = reach(row, bands)
    origin = -ncols if side else 2 * ncols
    span = slots_of(lambda lane: heads[place, HEAD, lane], 1 - side, low, high, bands)
    return [(tiles.at[place], span, (row, origin))]


def add_edge(out, heads, tiles, below, even_z, bands):
    cols = out.shape[2]
    row = jnp.where(below == 1, -HALF, bands * HALF)
    band = jnp.where(below == 1, 0, bands - 1)
    sources = []
    for t, half in ((0, even_z), (1, 0), (1, 1), (2, 1 - even_z)):
        column = (1 - t) * (2 * even_z - 1) * cols
        span = slots_of(lambda lane, t=t: heads[t, HEAD, lane], half, band, band, bands)
        sources.append((tiles.at[t], span, (row, column)))
    at = (0, HALF, 0, cols, EDGE_WINDOW)
    add_first(out, sources, *at, signed_wall=True, base=out)
    add_rest(out, sources, *at, signed_wall=True)


def transform(diag, shear, part):
    factors = jnp.concatenate([diag, shear, jnp.zeros((2, diag.shape[1]), jnp.float32)], axis=0).T
    a0, a1, a2 = (factors[:, k : k + 1] for k in range(3))
    b0, b1, b2 = (factors[:, 3 + k : 4 + k] for k in range(3))
    return a0 * part[0], b0 * part[0] + a1 * part[1], b1 * part[0] + b2 * part[1] + a2 * part[2]


def own_kernel(own_heads, own, out, *, bands, first):
    cols = out.shape[2]

    def add_block(block, carry):
        row = pl.multiple_of(block * ROWS, ROWS)
        sources = own_sources(own_heads, own, first + row, bands)
        add_first(out, sources, row, ROWS, 0, cols, WINDOW)
        add_rest(out, sources, row, ROWS, 0, cols, WINDOW)
        return carry

    lax.fori_loop(0, out.shape[1] // ROWS, add_block, 0)


def field_kernel(own_heads, heads, own, tiles, diag, shear, raw, out, acc, *, bands):
    cols = out.shape[2]
    ncols = cols // 2
    odd_z = own_heads[HEAD, 2] % 2
    whole_at = (0, ROWS, 0, cols, WINDOW)
    left_at = (0, ROWS, 0, ncols, WINDOW)
    right_at = (0, ROWS, ncols, ncols, WINDOW)

    def finish(block):
        at = pl.ds(pl.multiple_of(block * ROWS, ROWS), ROWS)
        for c, part in enumerate(transform(diag[:, at], shear[:, at], acc)):
            out[c, at, :] = part

    def add_block(block, with_own):
        row = pl.multiple_of(block * ROWS, ROWS)
        from_own = own_sources(own_heads, own, row, bands)
        from_left = side_sources(heads, tiles, 2 * odd_z, 0, row, ncols, bands)
        from_right = side_sources(heads, tiles, 2 - 2 * odd_z, 1, row, ncols, bands)
        finish(jnp.maximum(block - 1, 0))
        base, base_row = (acc, 0) if with_own else (raw, row)
        if with_own:
            add_first(acc, from_own, *whole_at)
        add_first(acc, from_left, *left_at, base=base, base_row=base_row)
        add_first(acc, from_right, *right_at, base=base, base_row=base_row)
        if with_own:
            add_rest(acc, from_own, *whole_at)
        add_rest(acc, from_left, *left_at)
        add_rest(acc, from_right, *right_at)

    nblocks, ready = out.shape[1] // ROWS, raw.shape[1] // ROWS
    acc[...] = jnp.zeros_like(acc)
    lax.fori_loop(0, ready, lambda k, x: (add_block(k, False), x)[1], 0)
    lax.fori_loop(ready, nblocks, lambda k, x: (add_block(k, True), x)[1], 0)
    finish(nblocks - 1)


def last_kernel(
    own_heads, up_heads, down_heads, near_y, far_y, over, known, field, diag, shear, mean, out, acc,
    *, bands, tiles_y, scale
):
    block = pl.program_id(0)
    rows = out.shape[1]
    nblocks = bands * HALF // rows
    at_y, odd_z = own_heads[HEAD, 1], own_heads[HEAD, 2] % 2
    odd_y = at_y % 2
    total = jnp.sum(jnp.maximum(known[...], over[...]).astype(jnp.float32), axis=1, keepdims=True)
    amplitude = jnp.sqrt(scale / total) * (1.5 / (HALF * HALF))
    at_block = pl.ds(pl.multiple_of(block * rows, rows), rows)
    out[...] = mean[:, at_block, :] + amplitude * field[:, at_block, :]

    def add_beyond(heads, tiles, below):
        acc[...] = jnp.zeros_like(acc)
        add_edge(acc, heads, tiles, below, 1 - odd_z, bands)
        first = pl.multiple_of(below * (bands * HALF - HALF), HALF)
        parts = transform(diag[:, pl.ds(first, HALF)], shear[:, pl.ds(first, HALF)], acc)
        at = pl.ds(pl.multiple_of(below * (rows - HALF), HALF), HALF)
        for c, part in enumerate(parts):
            out[c, at, :] += amplitude * part

    @pl.when(block == (1 - odd_y) * (nblocks - 1))
    def _():
        add_beyond(up_heads, near_y, 1 - odd_y)

    @pl.when((block == odd_y * (nblocks - 1)) & (at_y > 0) & (at_y < tiles_y - 1))
    def _():
        add_beyond(down_heads, far_y, odd_y)


def with_known(tile, known):
    wide = jnp.pad(known, ((0, 0), (0, tile.shape[1] - known.shape[1])))
    return jnp.where(jnp.arange(tile.shape[0])[:, None] == KNOWN, wide, tile)


def body(eddy_cells, eddy_signs, eddy_counts, stress_diag, stress_shear, mean_flow):
    slots = eddy_cells.shape[-1]
    _, rows, cols = mean_flow.shape
    tiles_y, tiles_z = lax.axis_size("gy"), lax.axis_size("gz")
    at_y, at_z = lax.axis_index("gy"), lax.axis_index("gz")
    assert cols == 2 * HALF and rows % (2 * ROWS) == 0 and slots % WINDOW == 0
    bands = rows // HALF
    assert START + 2 * bands < HALF
    assert tiles_z > 2 and tiles_z & (tiles_z - 1) == 0
    assert covers(pairs_skip(tiles_y) + [pairs_near(tiles_y), pairs_over(tiles_y, 2)], tiles_y)
    bands = rows // HALF
    assert START + 2 * bands < HALF
    assert covers([pairs_near(tiles_z), pairs_far(tiles_z)] + pairs_skip(tiles_z), tiles_z)
    assert covers(pairs_skip(tiles_y) + [pairs_near(tiles_y), pairs_over(tiles_y, 2)], tiles_y)

    vmem = pl.BlockSpec(memory_space=pltpu.VMEM)
    heads = pl.BlockSpec((8, HALF), lambda i: (0, 0), memory_space=pltpu.SMEM)
    field_block = pl.BlockSpec((3, ROWS, cols), lambda i: (0, i, 0))
    field_shape = jax.ShapeDtypeStruct((3, rows, cols), jnp.float32)
    edge_heads = pl.BlockSpec((3, 8, HALF), lambda i: (0, 0, 0), memory_space=pltpu.SMEM)
    macs = 3 * rows * cols * slots

    def cost(part, moved):
        return pl.CostEstimate(flops=int(2 * macs * part), transcendentals=0, bytes_accessed=int(4 * moved * 3 * rows * cols))

    count = eddy_counts.reshape(())
    lanes = -(-tiles_y * tiles_z // HALF) * HALF
    known = jnp.where(jnp.arange(lanes, dtype=jnp.int32)[None] == at_y * tiles_z + at_z, count, 0)
    for pairs in pairs_skip(tiles_y):
        known = jnp.maximum(known, lax.ppermute(known, "gy", pairs))
    own = pl.pallas_call(
        functools.partial(order_kernel, bands=bands, cols=cols),
        grid=(1,),
        in_specs=[pl.BlockSpec(memory_space=pltpu.SMEM), vmem, vmem],
        out_specs=vmem,
        out_shape=jax.ShapeDtypeStruct((8, slots), jnp.int32),
        cost_estimate=cost(0.3, 0.1),
        compiler_params=pltpu.CompilerParams(vmem_limit_bytes=24 << 20),
    )(eddy_counts, eddy_cells.reshape(2, slots), eddy_signs.reshape(3, slots))

    own = with_known(own, known)
    near_z = lax.ppermute(own, "gz", pairs_near(tiles_z))
    far_z = lax.ppermute(own, "gz", pairs_far(tiles_z))
    others = [known, near_z[KNOWN : KNOWN + 1, :lanes], far_z[KNOWN : KNOWN + 1, :lanes]]
    for by in range(2, tiles_z):
        if tiles_z != 4 or by == 2:
            others.append(lax.ppermute(known, "gz", pairs_over(tiles_z, by)))
    known = functools.reduce(jnp.maximum, others)
    row_of_tiles = jnp.stack([far_z, own, near_z])
    one = lax.ppermute(known, "gy", pairs_near(tiles_y))
    near_y = lax.ppermute(row_of_tiles, "gy", pairs_near(tiles_y))
    far_y = lax.ppermute(row_of_tiles, "gy", pairs_inner(tiles_y))

    half = rows // 2
    half_shape = jax.ShapeDtypeStruct((3, half, cols), jnp.float32)
    params = pltpu.CompilerParams(vmem_limit_bytes=24 << 20)
    acc = pltpu.VMEM((3, ROWS, cols), jnp.float32)
    raw = pl.pallas_call(
        functools.partial(own_kernel, bands=bands, first=0),
        grid=(1,),
        in_specs=[heads, vmem],
        out_specs=vmem,
        out_shape=half_shape,
        cost_estimate=cost(0.2, 0.5),
        compiler_params=params,
    )(own, own)

    known = jnp.maximum(known, one)
    over = lax.ppermute(known, "gy", pairs_over(tiles_y, 2))
    field = pl.pallas_call(
        functools.partial(field_kernel, bands=bands),
        grid=(1,),
        in_specs=[heads, edge_heads] + [vmem] * 5,
        out_specs=vmem,
        out_shape=field_shape,
        scratch_shapes=[acc],
        cost_estimate=cost(0.4, 1.0),
        compiler_params=params,
    )(own, row_of_tiles, own, row_of_tiles, stress_diag, stress_shear, raw)

    block_rows = LAST_ROWS
    last_block = pl.BlockSpec((3, block_rows, cols), lambda i: (0, i, 0))
    scale = rows * tiles_y * (cols * tiles_z) / (HALF * HALF)
    return pl.pallas_call(
        functools.partial(last_kernel, bands=bands, tiles_y=tiles_y, scale=scale),
        grid=(rows // block_rows,),
        in_specs=[heads] + [edge_heads] * 2 + [vmem] * 8,
        out_specs=last_block,
        out_shape=field_shape,
        scratch_shapes=[pltpu.VMEM((3, HALF, cols), jnp.float32)],
        cost_estimate=cost(0.3, 2.0),
        compiler_params=pltpu.CompilerParams(vmem_limit_bytes=24 << 20),
    )(
        own, near_y, far_y, near_y, far_y, over, known, field,
        stress_diag, stress_shear, mean_flow,
    )


def solution(mesh):
    in_specs = (
        P("gy", "gz", None, None),
        P("gy", "gz", None, None),
        P("gy", "gz"),
        P(None, "gy"),
        P(None, "gy"),
        P(None, "gy", "gz"),
    )

    return jax.shard_map(body, mesh=mesh, in_specs=in_specs, out_specs=P(None, "gy", "gz"), check_vma=False)
```

```python
import functools

import jax
import jax.numpy as jnp
from jax import lax
from jax.experimental import pallas as pl
from jax.experimental.pallas import tpu as pltpu
from jax.sharding import PartitionSpec as P


HALF = 128
ROWS = 512
LAST_ROWS = 256
WINDOW = 512
EDGE_WINDOW = 256
SORT = 256
KNOWN, HEAD, START = 5, 6, 3


def pairs_near(size):
    return [(i, i ^ 1) for i in range(size)]


def pairs_far(size):
    return [(i, (i + 1 if i % 2 else i - 1) % size) for i in range(size)]


def pairs_inner(size):
    return [(i, i + 1 if i % 2 else i - 1) for i in range(1, size - 1)]


def pairs_over(size, by):
    return [(i, i ^ by) for i in range(size)]


def pairs_skip(size):
    skips, by = [], 4
    while by < size:
        skips.append(pairs_over(size, by))
        by *= 2
    return skips


def covers(rounds, size):
    known = [{i} for i in range(size)]
    for pairs in rounds:
        known = [known[i] | known[dict(pairs)[i]] for i in range(size)]
    return size > 2 and all(len(k) == size for k in known)


def whole(values):
    return values.astype(jnp.float32).astype(jnp.bfloat16)


def cells_of(nrows, ncols):
    cells = whole(lax.broadcasted_iota(jnp.int32, (nrows, HALF), 0) - HALF)
    return jnp.concatenate([cells] * (ncols // HALF), axis=1)


def tent(cells, places, origin):
    near = whole(jnp.clip(places - (origin + HALF), -2 * HALF, 2 * HALF))
    return jnp.maximum(HALF - jnp.abs(cells - near), 0).astype(jnp.bfloat16)


def wall_profiles(tile, row, nrows):
    step = min(nrows, 2 * HALF)
    cells = cells_of(step, tile.shape[1])
    return jnp.concatenate([tent(cells, tile[0:1, :], row + r) for r in range(0, nrows, step)], axis=0)


def contract(a, b):
    return lax.dot_general(a, b, (((1,), (1,)), ((), ())), preferred_element_type=jnp.float32)


def order_kernel(count, cells, signs, out, *, bands, cols):
    slots = cells.shape[1]
    at_y, at_z = lax.axis_index("gy"), lax.axis_index("gz")
    nbuckets = -(-(2 * bands + 1) // 16) * 16
    places = jnp.concatenate([cells[0:1, :] - at_y * (bands * HALF), cells[1:2, :] - at_z * cols], axis=0)
    slot = lax.broadcasted_iota(jnp.int32, (1, slots), 1)
    bucket = jnp.where(slot < count[0, 0], (places[1:2] >> 7) * bands + (places[0:1] >> 7), 2 * bands)
    ids = lax.broadcasted_iota(jnp.int32, (nbuckets, HALF), 0)
    wide_ids = jnp.concatenate([ids] * (slots // HALF), axis=1)
    starts = jnp.sum((bucket < wide_ids).astype(jnp.float32), axis=1, keepdims=True)
    member = jnp.maximum(1 - jnp.abs(whole(wide_ids) - whole(bucket)), 0).astype(jnp.bfloat16)
    upto = lax.broadcasted_iota(jnp.int32, (SORT, SORT), 0) <= lax.broadcasted_iota(jnp.int32, (SORT, SORT), 1)
    pieces = [member[:, k : k + SORT] for k in range(0, slots, SORT)]
    so_far = lax.dot_general(
        jnp.concatenate(pieces, axis=0),
        whole(upto.astype(jnp.int32)),
        (((1,), (0,)), ((), ())),
        preferred_element_type=jnp.float32,
    )
    base = starts - 1
    ranks = []
    for k, piece in enumerate(pieces):
        part = so_far[k * nbuckets : (k + 1) * nbuckets, :]
        ranks.append(jnp.sum(piece.astype(jnp.float32) * (part + base), axis=0, keepdims=True))
        base = base + part[:, SORT - 1 : SORT]
    rank = jnp.concatenate(ranks, axis=1).astype(jnp.int32)

    live = jnp.where(slot < count[0, 0], signs[...], 0)
    parts = [places[0:1] >> 7, places[0:1] & (HALF - 1), places[1:2], live, jnp.zeros((2, slots), jnp.int32)]
    values = whole(jnp.concatenate(parts, axis=0))
    cells = jnp.concatenate([whole(lax.broadcasted_iota(jnp.int32, (SORT, HALF), 0))] * (slots // HALF), axis=1)
    for k in range(slots // SORT):
        local = whole(jnp.where(rank // SORT == k, rank % SORT, -1))
        chosen = jnp.maximum(1 - jnp.abs(cells - local), 0).astype(jnp.bfloat16)
        got = contract(values, chosen).astype(jnp.int32)
        at = slice(k * SORT, (k + 1) * SORT)
        out[0:1, at] = got[0:1] * HALF + got[1:2]
        out[1:5, at] = got[2:6]
    out[KNOWN:, :] = jnp.zeros((8 - KNOWN, slots), jnp.int32)
    lane = lax.broadcasted_iota(jnp.int32, (nbuckets, HALF), 1)
    firsts = jnp.sum(jnp.where(lane == ids + START, starts, 0.0), axis=0, keepdims=True).astype(jnp.int32)
    place = jnp.where(lane[0:1] == 0, count[0, 0], jnp.where(lane[0:1] == 1, at_y, at_z))
    out[HEAD : HEAD + 1, :HALF] = jnp.where(lane[0:1] < START, place, firsts)


def slots_of(head, half, low, high, bands):
    return head(START + half * bands + low), head(START + half * bands + high + 1)


def profiles(tile_ref, first, span, origin, nrows, ncols, size, signed_wall):
    at = pl.multiple_of(jnp.minimum(first, tile_ref.shape[-1] - size), HALF)
    tile = tile_ref[:, pl.ds(at, size)]
    slot = at + lax.broadcasted_iota(jnp.int32, (1, size), 1)
    inside = (slot >= jnp.maximum(span[0], first)) & (slot < jnp.minimum(span[1], first + size))
    signs = whole(jnp.where(inside, tile[2:5, :], 0))
    wall = wall_profiles(tile, origin[0], nrows)
    along = tent(cells_of(ncols, size), tile[1:2, :], origin[1])
    if signed_wall:
        return jnp.concatenate([wall * signs[c : c + 1, :] for c in range(3)], axis=0), along
    return wall, jnp.concatenate([along * signs[c : c + 1, :] for c in range(3)], axis=0)


def add_windows(out, sources, firsts, at_row, nrows, at_col, ncols, size, signed_wall, base, base_row):
    pairs = [profiles(s[0], f, s[1], s[2], nrows, ncols, size, signed_wall) for s, f in zip(sources, firsts)]
    wall, along = (jnp.concatenate(x, axis=1) if len(x) > 1 else x[0] for x in zip(*pairs))
    part = contract(wall, along)
    for c in range(3):
        piece = part[c * nrows : (c + 1) * nrows] if signed_wall else part[:, c * ncols : (c + 1) * ncols]
        if base is not None:
            piece = piece + base[c, pl.ds(base_row, nrows), pl.ds(at_col, ncols)]
        out[c, pl.ds(at_row, nrows), pl.ds(at_col, ncols)] = piece


def first_window(source):
    return source[1][0] // HALF * HALF


def add_first(out, sources, at_row, nrows, at_col, ncols, size, signed_wall=False, base=None, base_row=0):
    firsts = [first_window(s) for s in sources]
    add_windows(out, sources, firsts, at_row, nrows, at_col, ncols, size, signed_wall, base, base_row)


def add_rest(out, sources, at_row, nrows, at_col, ncols, size, signed_wall=False):
    for source in sources:
        first = first_window(source)

        def more(k, carry, source=source, first=first):
            start = [first + k * size]
            add_windows(out, [source], start, at_row, nrows, at_col, ncols, size, signed_wall, out, at_row)
            return carry

        lax.fori_loop(1, (source[1][1] - first + size - 1) // size, more, 0)


def reach(row, bands):
    band = row // HALF
    return jnp.maximum(band - 1, 0), jnp.minimum(band + ROWS // HALF, bands - 1)


def head_of(heads):
    return lambda lane: heads[HEAD, lane]


def own_sources(heads, tile, row, bands):
    low, high = reach(row, bands)
    return [(tile, slots_of(head_of(heads), half, low, high, bands), (row, 0)) for half in range(2)]


def side_sources(heads, tiles, place, side, row, ncols, bands):
    low, high = reach(row, bands)
    origin = -ncols if side else 2 * ncols
    span = slots_of(lambda lane: heads[place, HEAD, lane], 1 - side, low, high, bands)
    return [(tiles.at[place], span, (row, origin))]


def add_edge(out, heads, tiles, below, even_z, bands):
    cols = out.shape[2]
    row = jnp.where(below == 1, -HALF, bands * HALF)
    band = jnp.where(below == 1, 0, bands - 1)
    sources = []
    for t, half in ((0, even_z), (1, 0), (1, 1), (2, 1 - even_z)):
        column = (1 - t) * (2 * even_z - 1) * cols
        span = slots_of(lambda lane, t=t: heads[t, HEAD, lane], half, band, band, bands)
        sources.append((tiles.at[t], span, (row, column)))
    at = (0, HALF, 0, cols, EDGE_WINDOW)
    add_first(out, sources, *at, signed_wall=True, base=out)
    add_rest(out, sources, *at, signed_wall=True)


def transform(diag, shear, part):
    factors = jnp.concatenate([diag, shear, jnp.zeros((2, diag.shape[1]), jnp.float32)], axis=0).T
    a0, a1, a2 = (factors[:, k : k + 1] for k in range(3))
    b0, b1, b2 = (factors[:, 3 + k : 4 + k] for k in range(3))
    return a0 * part[0], b0 * part[0] + a1 * part[1], b1 * part[0] + b2 * part[1] + a2 * part[2]


def own_kernel(own_heads, own, out, *, bands, first):
    cols = out.shape[2]

    def add_block(block, carry):
        row = pl.multiple_of(block * ROWS, ROWS)
        sources = own_sources(own_heads, own, first + row, bands)
        add_first(out, sources, row, ROWS, 0, cols, WINDOW)
        add_rest(out, sources, row, ROWS, 0, cols, WINDOW)
        return carry

    lax.fori_loop(0, out.shape[1] // ROWS, add_block, 0)


def field_kernel(own_heads, heads, own, tiles, diag, shear, raw, out, acc, *, bands):
    cols = out.shape[2]
    ncols = cols // 2
    odd_z = own_heads[HEAD, 2] % 2
    whole_at = (0, ROWS, 0, cols, WINDOW)
    left_at = (0, ROWS, 0, ncols, WINDOW)
    right_at = (0, ROWS, ncols, ncols, WINDOW)

    def finish(block):
        at = pl.ds(pl.multiple_of(block * ROWS, ROWS), ROWS)
        for c, part in enumerate(transform(diag[:, at], shear[:, at], acc)):
            out[c, at, :] = part

    def add_block(block, with_own):
        row = pl.multiple_of(block * ROWS, ROWS)
        from_own = own_sources(own_heads, own, row, bands)
        from_left = side_sources(heads, tiles, 2 * odd_z, 0, row, ncols, bands)
        from_right = side_sources(heads, tiles, 2 - 2 * odd_z, 1, row, ncols, bands)
        finish(jnp.maximum(block - 1, 0))
        base, base_row = (acc, 0) if with_own else (raw, row)
        if with_own:
            add_first(acc, from_own, *whole_at)
        add_first(acc, from_left, *left_at, base=base, base_row=base_row)
        add_first(acc, from_right, *right_at, base=base, base_row=base_row)
        if with_own:
            add_rest(acc, from_own, *whole_at)
        add_rest(acc, from_left, *left_at)
        add_rest(acc, from_right, *right_at)

    nblocks, ready = out.shape[1] // ROWS, raw.shape[1] // ROWS
    acc[...] = jnp.zeros_like(acc)
    lax.fori_loop(0, ready, lambda k, x: (add_block(k, False), x)[1], 0)
    lax.fori_loop(ready, nblocks, lambda k, x: (add_block(k, True), x)[1], 0)
    finish(nblocks - 1)


def last_kernel(
    own_heads, up_heads, down_heads, near_y, far_y, over, known, field, diag, shear, mean, out, acc, ready, sems,
    *, bands, tiles_y, scale
):
    rows = LAST_ROWS
    nblocks = bands * HALF // rows
    at_y, odd_z = own_heads[HEAD, 1], own_heads[HEAD, 2] % 2
    odd_y = at_y % 2
    total = jnp.sum(jnp.maximum(known[...], over[...]).astype(jnp.float32), axis=1, keepdims=True)
    amplitude = jnp.sqrt(scale / total) * (1.5 / (HALF * HALF))

    def copy_of(block):
        at = slice(block * rows, (block + 1) * rows)
        return pltpu.make_async_copy(ready.at[:, at, :], out.at[:, at, :], sems.at[block])

    def fill(block):
        at = slice(block * rows, (block + 1) * rows)
        ready[:, at, :] = mean[:, at, :] + amplitude * field[:, at, :]

    def add_beyond(heads, tiles, below):
        acc[...] = jnp.zeros_like(acc)
        add_edge(acc, heads, tiles, below, 1 - odd_z, bands)
        at = pl.ds(pl.multiple_of(below * (bands * HALF - HALF), HALF), HALF)
        for c, part in enumerate(transform(diag[:, at], shear[:, at], acc)):
            ready[c, at, :] += amplitude * part

    for block in range(1, nblocks - 1):
        fill(block)
        copy_of(block).start()
    fill(0)
    fill(nblocks - 1)
    add_beyond(up_heads, near_y, 1 - odd_y)

    @pl.when((at_y > 0) & (at_y < tiles_y - 1))
    def _():
        add_beyond(down_heads, far_y, odd_y)

    copy_of(0).start()
    copy_of(nblocks - 1).start()
    for block in range(nblocks):
        copy_of(block).wait()


def with_known(tile, known):
    wide = jnp.pad(known, ((0, 0), (0, tile.shape[1] - known.shape[1])))
    return jnp.where(jnp.arange(tile.shape[0])[:, None] == KNOWN, wide, tile)


def body(eddy_cells, eddy_signs, eddy_counts, stress_diag, stress_shear, mean_flow):
    slots = eddy_cells.shape[-1]
    _, rows, cols = mean_flow.shape
    tiles_y, tiles_z = lax.axis_size("gy"), lax.axis_size("gz")
    at_y, at_z = lax.axis_index("gy"), lax.axis_index("gz")
    assert cols == 2 * HALF and rows % (2 * ROWS) == 0 and slots % WINDOW == 0
    bands = rows // HALF
    assert START + 2 * bands < HALF
    assert tiles_z > 2 and tiles_z & (tiles_z - 1) == 0
    assert covers(pairs_skip(tiles_y) + [pairs_near(tiles_y), pairs_over(tiles_y, 2)], tiles_y)
    bands = rows // HALF
    assert START + 2 * bands < HALF
    assert covers([pairs_near(tiles_z), pairs_far(tiles_z)] + pairs_skip(tiles_z), tiles_z)
    assert covers(pairs_skip(tiles_y) + [pairs_near(tiles_y), pairs_over(tiles_y, 2)], tiles_y)

    vmem = pl.BlockSpec(memory_space=pltpu.VMEM)
    heads = pl.BlockSpec((8, HALF), lambda i: (0, 0), memory_space=pltpu.SMEM)
    field_block = pl.BlockSpec((3, ROWS, cols), lambda i: (0, i, 0))
    field_shape = jax.ShapeDtypeStruct((3, rows, cols), jnp.float32)
    edge_heads = pl.BlockSpec((3, 8, HALF), lambda i: (0, 0, 0), memory_space=pltpu.SMEM)
    macs = 3 * rows * cols * slots

    def cost(part, moved):
        return pl.CostEstimate(flops=int(2 * macs * part), transcendentals=0, bytes_accessed=int(4 * moved * 3 * rows * cols))

    count = eddy_counts.reshape(())
    lanes = -(-tiles_y * tiles_z // HALF) * HALF
    known = jnp.where(jnp.arange(lanes, dtype=jnp.int32)[None] == at_y * tiles_z + at_z, count, 0)
    for pairs in pairs_skip(tiles_y):
        known = jnp.maximum(known, lax.ppermute(known, "gy", pairs))
    own = pl.pallas_call(
        functools.partial(order_kernel, bands=bands, cols=cols),
        grid=(1,),
        in_specs=[pl.BlockSpec(memory_space=pltpu.SMEM), vmem, vmem],
        out_specs=vmem,
        out_shape=jax.ShapeDtypeStruct((8, slots), jnp.int32),
        cost_estimate=cost(0.3, 0.1),
        compiler_params=pltpu.CompilerParams(vmem_limit_bytes=24 << 20),
    )(eddy_counts, eddy_cells.reshape(2, slots), eddy_signs.reshape(3, slots))

    own = with_known(own, known)
    near_z = lax.ppermute(own, "gz", pairs_near(tiles_z))
    far_z = lax.ppermute(own, "gz", pairs_far(tiles_z))
    others = [known, near_z[KNOWN : KNOWN + 1, :lanes], far_z[KNOWN : KNOWN + 1, :lanes]]
    for by in range(2, tiles_z):
        if tiles_z != 4 or by == 2:
            others.append(lax.ppermute(known, "gz", pairs_over(tiles_z, by)))
    known = functools.reduce(jnp.maximum, others)
    row_of_tiles = jnp.stack([far_z, own, near_z])
    one = lax.ppermute(known, "gy", pairs_near(tiles_y))
    near_y = lax.ppermute(row_of_tiles, "gy", pairs_near(tiles_y))
    far_y = lax.ppermute(row_of_tiles, "gy", pairs_inner(tiles_y))

    half = rows // 2
    half_shape = jax.ShapeDtypeStruct((3, half, cols), jnp.float32)
    params = pltpu.CompilerParams(vmem_limit_bytes=24 << 20)
    acc = pltpu.VMEM((3, ROWS, cols), jnp.float32)
    raw = pl.pallas_call(
        functools.partial(own_kernel, bands=bands, first=0),
        grid=(1,),
        in_specs=[heads, vmem],
        out_specs=vmem,
        out_shape=half_shape,
        cost_estimate=cost(0.2, 0.5),
        compiler_params=params,
    )(own, own)

    known = jnp.maximum(known, one)
    over = lax.ppermute(known, "gy", pairs_over(tiles_y, 2))
    field = pl.pallas_call(
        functools.partial(field_kernel, bands=bands),
        grid=(1,),
        in_specs=[heads, edge_heads] + [vmem] * 5,
        out_specs=vmem,
        out_shape=field_shape,
        scratch_shapes=[acc],
        cost_estimate=cost(0.4, 1.0),
        compiler_params=params,
    )(own, row_of_tiles, own, row_of_tiles, stress_diag, stress_shear, raw)

    scale = rows * tiles_y * (cols * tiles_z) / (HALF * HALF)
    return pl.pallas_call(
        functools.partial(last_kernel, bands=bands, tiles_y=tiles_y, scale=scale),
        grid=(1,),
        in_specs=[heads] + [edge_heads] * 2 + [vmem] * 8,
        out_specs=pl.BlockSpec(memory_space=pltpu.HBM),
        out_shape=field_shape,
        scratch_shapes=[
            pltpu.VMEM((3, HALF, cols), jnp.float32),
            pltpu.VMEM((3, rows, cols), jnp.float32),
            pltpu.SemaphoreType.DMA((rows // LAST_ROWS,)),
        ],
        cost_estimate=cost(0.3, 2.0),
        compiler_params=pltpu.CompilerParams(vmem_limit_bytes=24 << 20),
    )(
        own, near_y, far_y, near_y, far_y, over, known, field,
        stress_diag, stress_shear, mean_flow,
    )


def solution(mesh):
    in_specs = (
        P("gy", "gz", None, None),
        P("gy", "gz", None, None),
        P("gy", "gz"),
        P(None, "gy"),
        P(None, "gy"),
        P(None, "gy", "gz"),
    )

    return jax.shard_map(body, mesh=mesh, in_specs=in_specs, out_specs=P(None, "gy", "gz"), check_vma=False)
```
